32 devices in a mesh: rows: 8 (over z, y), grp: 4 (over x, core).
Axes of the slice: x: 2, y: 2, z: 4, core: 2. Of those that a mesh axis runs over, the one named last changes fastest.
Arguments:
- owner: int32 [1024, 24, 3], P('rows', 'grp'), may hold values from 0 to 7, as said below
- offset: int32 [1024, 24, 3], P('rows', 'grp'), may hold values from 0 to 511
- tables: float32 [12, 4096, 128], P('grp', 'rows'), may hold values from -6 to 6
- w_first: bfloat16 [3072, 1024], P('grp'), may hold values from -0.109375 to 0.109375
- b_first: float32 [1024], replicated, may hold values from -3 to 3
- w_out: float32 [1024], replicated, may hold values from -0.1875 to 0.1875
- labels: int32 [1024], P('rows'), may hold values 0 or 1
Outputs:
- table_grad: float32 [12, 4096, 128], P('grp', 'rows')
- losses: float32 [1024], P(('rows', 'grp'))
The draws below stay inside these ranges and needn't reach their ends.
Inputs may be any that keep to these rules, and one draw needn't show every extreme that they name: Of the lookups of one device (its 128 samples and 6 features, all three hashes) at most 1032 name one owner, and in every draw some owner gets exactly 1032. Among the lookups of one device to one owner for one table, at most 114 distinct offsets occur, and that bound is reached in every draw.
All inputs are finite; a program needn't handle non-finite values. No bound on the sum of `labels` on one device may be relied on, other than what follows from the above.
Results may differ from the reference program's by a relative error of at most 0.005.
Values may be sent and summed in bfloat16 or wider, within the bound.
A program may use at most 64 MiB of HBM per device.

```python
import jax
import jax.numpy as jnp
from jax import lax

E = 128
H = 1024
F_GRP = 6
B_DEV = 128
ROWS_DEV = 512
BATCH = 1024
FEATURES = 24
TAB_ROWS = 4096
HOTK = 344
UNIQ = 114
N_GRP = 4


def layout_pair(key):
    row_devices = BATCH // B_DEV
    group_devices = FEATURES // F_GRP
    block_size = B_DEV * F_GRP
    base_key = jax.random.fold_in(key, 7001)

    def device_block(block_key):
        subkeys = jax.random.split(block_key, 4)
        hot_owner = jax.random.randint(subkeys[0], (), 0, row_devices)
        rank_of = jnp.stack([jax.random.permutation(jax.random.fold_in(subkeys[1], column), block_size) for column in range(3)], axis=1).astype(jnp.int32)
        spread_owner = (hot_owner + 1 + (rank_of - HOTK) % (row_devices - 1)) % row_devices
        owners = jnp.where(rank_of < HOTK, hot_owner, spread_owner).astype(jnp.int32)
        pool_pick = jnp.where(rank_of < HOTK, rank_of % UNIQ, jax.random.randint(subkeys[2], (block_size, 3), 0, UNIQ))
        pool_base = jax.random.randint(subkeys[3], (row_devices, 3), 0, ROWS_DEV)
        pool_step = ROWS_DEV // UNIQ
        chosen_base = pool_base[owners, jnp.arange(3, dtype=jnp.int32)[None, :]]
        offsets = (chosen_base + pool_pick * pool_step) % ROWS_DEV
        return (owners.reshape(B_DEV, F_GRP, 3), offsets.astype(jnp.int32).reshape(B_DEV, F_GRP, 3))
    block_keys = jax.random.split(base_key, row_devices * group_devices)
    owners, offsets = jax.vmap(device_block)(block_keys)
    owners = owners.reshape(row_devices, group_devices, B_DEV, F_GRP, 3).transpose(0, 2, 1, 3, 4).reshape(BATCH, FEATURES, 3)
    offsets = offsets.reshape(row_devices, group_devices, B_DEV, F_GRP, 3).transpose(0, 2, 1, 3, 4).reshape(BATCH, FEATURES, 3)
    return (owners, offsets)


def draw_owner(key, part):
    return layout_pair(key)[0]


def draw_offset(key, part):
    return layout_pair(key)[1]


def place_ends(result, stream_key, least, top_value):
    longest = result.shape.index(max(result.shape))
    spots = []
    for shift in (0, 1):
        where = [jax.random.randint(jax.random.fold_in(stream_key, axis), (), 0, length) for axis, length in enumerate(result.shape)]
        where[longest] = (where[longest] + shift) % result.shape[longest]
        spots.append(tuple(where))
    return result.at[spots[0]].set(least).at[spots[1]].set(top_value)


def levels(rng, dims, cuts, low, largest):
    def one(dim, parts):
        draws = jax.random.uniform(jax.random.fold_in(jax.random.fold_in(rng, 6), dim), (parts,), jnp.float32, low / len(cuts), largest / len(cuts))
        return jnp.repeat(jnp.exp(draws), dims[dim] // parts).reshape((-1,) + (1,) * (len(dims) - dim - 1))

    level = one(*cuts[0])
    for cut in cuts[1:]:
        level = level * one(*cut)
    return level


def normal_values(key, shape, scale, limit, cuts=(), kind=jnp.bfloat16):
    values = jax.random.normal(key, shape, jnp.float32) * scale
    if len(cuts) > 0:
        values = levels(key, shape, cuts, -0.22, 0.18) * values
    return jnp.clip(values, min=-limit, max=limit).astype(kind)


def setup_inputs(seed: int = 0) -> dict:
    key_of = jax.random.split(jax.random.key(seed), 8)
    return {
        "owner": draw_owner(jax.random.fold_in(key_of[7], 71), 0),
        "offset": draw_offset(jax.random.fold_in(key_of[7], 71), 0),
        "tables": normal_values(key_of[2], (3 * N_GRP, TAB_ROWS, E), 1.0, 6.0, ((0, 4), (1, 8)), jnp.float32),
        "w_first": normal_values(key_of[3], (FEATURES * E, H), (FEATURES * E) ** -0.5, 0.109375, ((0, 4),)),
        "b_first": normal_values(key_of[4], (H,), 0.5, 3.0, (), jnp.float32),
        "w_out": normal_values(key_of[5], (H,), H ** -0.5, 0.1875, (), jnp.float32),
        "labels": place_ends((jax.random.randint(key_of[6], (BATCH,), 0, 2) < 1).astype(jnp.int32), jax.random.fold_in(key_of[6], 1), 0, 1),
    }


def reference(owner, offset, tables, w_first, b_first, w_out, labels):
    table_kind = jnp.arange(3, dtype=jnp.int32)
    feature_group = jnp.arange(FEATURES, dtype=jnp.int32) // F_GRP
    table_id = jnp.broadcast_to(feature_group[None, :, None] * 3 + table_kind[None, None, :], owner.shape).astype(jnp.int32)
    row_id = (owner * ROWS_DEV + offset).astype(jnp.int32)
    looked_low = tables[table_id, row_id].astype(jnp.bfloat16)
    looked = lax.optimization_barrier(looked_low).astype(jnp.float32)
    embedded = looked[:, :, 0] * looked[:, :, 1] + looked[:, :, 2]
    features = embedded.reshape(BATCH, FEATURES * E).astype(jnp.bfloat16)
    pre_act = jnp.dot(features, w_first, preferred_element_type=jnp.float32) + b_first
    gate_sig = jax.nn.sigmoid(pre_act)
    logits = jnp.sum(pre_act * gate_sig * w_out, axis=1)
    targets = labels.astype(jnp.float32)
    losses = jax.nn.softplus(logits) - targets * logits
    grad_logit = jax.nn.sigmoid(logits) - targets
    grad_pre = (grad_logit[:, None] * w_out * (gate_sig * (1.0 + pre_act * (1.0 - gate_sig)))).astype(jnp.bfloat16)
    grad_emb = jnp.dot(grad_pre, w_first.T, preferred_element_type=jnp.float32).reshape(BATCH, FEATURES, E)
    row_grads = jnp.stack([grad_emb * looked[:, :, 1], grad_emb * looked[:, :, 0], grad_emb], axis=2)
    table_grad = jnp.zeros((3 * N_GRP, TAB_ROWS, E), jnp.float32).at[table_id, row_id].add(row_grads)
    return table_grad, losses
```

```python
import functools

import jax
import jax.numpy as jnp
from jax import lax
from jax.experimental import pallas as pl
from jax.experimental.pallas import tpu as pltpu
from jax.sharding import PartitionSpec as P

BF16 = jnp.bfloat16
F32 = jnp.float32


def iota(shape, dim):
    return lax.broadcasted_iota(jnp.int32, shape, dim)


def ones_where(mask):
    return jnp.where(mask, 1.0, 0.0).astype(BF16)


def mm(a, b):
    return jnp.dot(a, b, preferred_element_type=F32)


def kernel(
    R, G, cap, fgrp,
    idx_ref, tab_hbm, w_hbm, b_ref, wo_ref,
    tg_ref, loss_ref,
    tab, tb, w, col, of, ranked_bf, req_send, req_recv, fet_send, rows, looked,
    p_ref, pt_ref, st_ref, part_f32, part_send, part_recv, gp, rg, g_send, g_recv,
    local_sem, ss0, rs0, ss1, rs1, ss2, rs2, ssp, rsp, ssg, rsg,
):
    me = lax.axis_index("rows")
    mg = lax.axis_index("grp")
    n_rows = tab.shape[1]
    emb = tab.shape[2]
    nl = idx_ref.shape[1]
    per = nl // 3
    bdev = per // fgrp
    share = bdev // G
    r8 = R * 8
    slots = R * cap

    barrier = pltpu.get_barrier_semaphore()

    def up(k):
        return lax.rem(me + k, R)

    def down(k):
        return lax.rem(me - k + R, R)

    def gup(k):
        return lax.rem(mg + k, G)

    @pl.loop(1, R)
    def _(k):
        pl.semaphore_signal(barrier, inc=1, device_id={"rows": up(k)})

    @pl.loop(1, G)
    def _(k):
        pl.semaphore_signal(barrier, inc=1, device_id={"grp": gup(k)})

    tab_copy = pltpu.make_async_copy(tab_hbm, tab, local_sem.at[0])
    w_copy = pltpu.make_async_copy(w_hbm, w, local_sem.at[1])
    tab_copy.start()
    w_copy.start()

    for j in range(nl // 128):
        col[pl.ds(j * 128, 128), :] = idx_ref[:, pl.ds(j * 128, 128)].T
    for t in range(3):
        at = pl.ds(t * per, per)
        of[at, :] = ones_where(iota((per, n_rows), 1) == col[at, 1:2])
    owner_hot = ones_where(iota((r8, nl), 0) == idx_ref[0:1, :])
    present = mm(owner_hot, of[...]) > 0.5
    before = ones_where(iota((n_rows, n_rows), 0) < iota((n_rows, n_rows), 1))
    ranked = jnp.where(present, mm(ones_where(present), before), -1.0)
    ranked_bf[...] = ranked.astype(BF16)
    req_send[...] = ranked.reshape(R, 8, n_rows)

    pl.semaphore_wait(barrier, R - 1 + G - 1)

    def req_copy(k):
        return pltpu.make_async_remote_copy(
            req_send.at[up(k)], req_recv.at[me], ss0.at[k], rs0.at[k],
            device_id={"rows": up(k)}, device_id_type=pl.DeviceIdType.MESH,
        )

    @pl.loop(1, R)
    def _(k):
        req_copy(k).start()

    tab_copy.wait()
    tb[...] = tab[...].astype(BF16)
    req_recv[me] = req_send[me]

    for t in range(3):
        at = pl.ds(t * per, per)
        own_hot = ones_where(iota((per, r8), 1) == col[at, 0:1])
        picked = mm(own_hot, ranked_bf[...]) * of[at, :].astype(F32)
        slot = jnp.sum(picked, axis=1, keepdims=True) + col[at, 3:4].astype(F32)
        looked[t] = jnp.broadcast_to(slot, (per, emb))

    def fetch(src):
        for t in range(3):
            pick = ones_where(
                iota((cap, n_rows), 0).astype(F32) == req_recv[src, pl.ds(t, 1), :]
            )
            fet_send[src, t] = mm(pick, tb[t]).astype(BF16)

    def row_copy(k):
        return pltpu.make_async_remote_copy(
            fet_send.at[down(k)], rows.at[me], ss1.at[k], rs1.at[k],
            device_id={"rows": down(k)}, device_id_type=pl.DeviceIdType.MESH,
        )

    @pl.loop(1, R)
    def _(k):
        req_copy(k).wait_recv()
        fetch(down(k))
        row_copy(k).start()

    fetch(me)
    rows[me] = fet_send[me]

    lane_slot = iota((per, slots), 1).astype(F32)
    for t in range(3):
        slot = looked[t]
        p_ref[t] = ones_where(lane_slot == slot[:, 0:1])
        slot_row = slot.T[0:1, :]
        pt_ref[t] = ones_where(iota((slots, per), 0).astype(F32) == slot_row)
    req_cols = req_recv[...].reshape(r8, n_rows).T.astype(BF16)
    row_i = iota((r8, slots), 0)
    col_j = iota((r8, slots), 1)
    first = (row_i >> 3) * cap
    slot_in = (iota((n_rows, slots), 1) & (cap - 1)).astype(F32)
    for t in range(3):
        spread = ones_where(((row_i & 7) == t) & (col_j >= first) & (col_j < first + cap))
        st_ref[t] = ones_where(mm(req_cols, spread) == slot_in)

    @pl.loop(1, R)
    def _(k):
        row_copy(k).wait_recv()

    for t in range(3):
        looked[t] = mm(p_ref[t], rows[:, t].reshape(slots, emb))
    embedded = (looked[0] * looked[1] + looked[2]).astype(BF16)
    features = jnp.concatenate(
        [embedded[f * bdev : (f + 1) * bdev] for f in range(fgrp)], axis=1
    )
    w_copy.wait()
    partial = mm(features, w[...])
    hidden = partial.shape[1]
    part_f32[...] = partial.reshape(G, share, hidden)
    part_send[...] = partial.astype(BF16).reshape(G, share, hidden)

    def part_copy(k):
        return pltpu.make_async_remote_copy(
            part_send.at[gup(k)], part_recv.at[k], ssp.at[k], rsp.at[k],
            device_id={"grp": gup(k)}, device_id_type=pl.DeviceIdType.MESH,
        )

    for k in range(1, G):
        part_copy(k).start()
    pre = part_f32[mg] + b_ref[...]
    for k in range(1, G):
        part_copy(k).wait_recv()
        pre = pre + part_recv[k].astype(F32)
    sig = jax.nn.sigmoid(pre)
    w_out = wo_ref[...]
    logits = jnp.sum(pre * sig * w_out, axis=1, keepdims=True)
    targets = col[pl.ds(pl.multiple_of(mg * share, share), share), 2:3].astype(F32)
    grad_logit = jax.nn.sigmoid(logits) - targets
    gp[mg] = (grad_logit * w_out * (sig * (1.0 + pre * (1.0 - sig)))).astype(BF16)

    def gp_copy(k):
        return pltpu.make_async_remote_copy(
            gp.at[mg], gp.at[mg], ssg.at[k], rsg.at[k],
            device_id={"grp": gup(k)}, device_id_type=pl.DeviceIdType.MESH,
        )

    for k in range(1, G):
        gp_copy(k).start()
    losses = (
        jnp.maximum(logits, 0.0) + jnp.log1p(jnp.exp(-jnp.abs(logits))) - targets * logits
    )
    diag = iota((share, share), 0) == iota((share, share), 1)
    loss_ref[...] = jnp.sum(jnp.where(diag, losses, 0.0), axis=0, keepdims=True)
    for k in range(1, G):
        gp_copy(k).wait_recv()

    grad_emb = lax.dot_general(
        gp[...].reshape(bdev, hidden), w[...], (((1,), (1,)), ((), ())),
        preferred_element_type=F32,
    )
    grad_rows = jnp.concatenate(
        [grad_emb[:, f * emb : (f + 1) * emb] for f in range(fgrp)], axis=0
    )
    rg[0] = (grad_rows * looked[1]).astype(BF16)
    rg[1] = (grad_rows * looked[0]).astype(BF16)
    rg[2] = grad_rows.astype(BF16)

    def collect(dst):
        for t in range(3):
            hot = pt_ref[t, pl.ds(pl.multiple_of(dst * cap, cap), cap), :]
            g_send[dst, t] = mm(hot, rg[t]).astype(BF16)

    def grad_copy(k):
        return pltpu.make_async_remote_copy(
            g_send.at[up(k)], g_recv.at[me], ss2.at[k], rs2.at[k],
            device_id={"rows": up(k)}, device_id_type=pl.DeviceIdType.MESH,
        )

    @pl.loop(1, R)
    def _(k):
        collect(up(k))
        grad_copy(k).start()

    collect(me)
    g_recv[me] = g_send[me]

    @pl.loop(1, R)
    def _(k):
        req_copy(k).wait_send()
        row_copy(k).wait_send()

    for k in range(1, G):
        part_copy(k).wait_send()
        gp_copy(k).wait_send()

    @pl.loop(1, R)
    def _(k):
        grad_copy(k).wait_recv()

    for t in range(3):
        tg_ref[t] = mm(st_ref[t], g_recv[:, t].reshape(slots, emb))

    @pl.loop(1, R)
    def _(k):
        grad_copy(k).wait_send()


def body(owner, offset, tables, w_first, b_first, w_out, labels):
    R, G = lax.axis_size("rows"), lax.axis_size("grp")
    bdev, fgrp = owner.shape[0], owner.shape[1]
    n_rows, emb = tables.shape[1], tables.shape[2]
    hidden = w_first.shape[1]
    per = bdev * fgrp
    nl = 3 * per
    hot_count = 8 * (per * 7 // (16 * R)) + 8
    cap = 16
    while cap < hot_count // 3:
        cap *= 2
    share = bdev // G
    slots = R * cap

    owner_rows = owner.transpose(2, 1, 0).reshape(1, nl)
    offset_rows = offset.transpose(2, 1, 0).reshape(1, nl)
    kind = jnp.arange(nl, dtype=jnp.int32)[None, :] // per
    label_row = jnp.pad(labels, (0, nl - bdev))[None, :]
    idx = jnp.concatenate(
        [owner_rows * 8 + kind, offset_rows, label_row, owner_rows * cap,
         jnp.zeros((4, nl), jnp.int32)],
        axis=0,
    )
    vmem = pl.BlockSpec(memory_space=pltpu.VMEM)
    hbm = pl.BlockSpec(memory_space=pl.ANY)
    sems = pltpu.SemaphoreType.DMA
    table_grad, losses = pl.pallas_call(
        functools.partial(kernel, R, G, cap, fgrp),
        out_shape=(
            jax.ShapeDtypeStruct((3, n_rows, emb), F32),
            jax.ShapeDtypeStruct((1, share), F32),
        ),
        in_specs=[vmem, hbm, hbm, vmem, vmem],
        out_specs=(vmem, vmem),
        scratch_shapes=[
            pltpu.VMEM((3, n_rows, emb), F32),
            pltpu.VMEM((3, n_rows, emb), BF16),
            pltpu.VMEM(w_first.shape, BF16),
            pltpu.VMEM((nl, 8), jnp.int32),
            pltpu.VMEM((nl, n_rows), BF16),
            pltpu.VMEM((R * 8, n_rows), BF16),
            pltpu.VMEM((R, 8, n_rows), F32),
            pltpu.VMEM((R, 8, n_rows), F32),
            pltpu.VMEM((R, 3, cap, emb), BF16),
            pltpu.VMEM((R, 3, cap, emb), BF16),
            pltpu.VMEM((3, per, emb), F32),
            pltpu.VMEM((3, per, slots), BF16),
            pltpu.VMEM((3, slots, per), BF16),
            pltpu.VMEM((3, n_rows, slots), BF16),
            pltpu.VMEM((G, share, hidden), F32),
            pltpu.VMEM((G, share, hidden), BF16),
            pltpu.VMEM((G, share, hidden), BF16),
            pltpu.VMEM((G, share, hidden), BF16),
            pltpu.VMEM((3, per, emb), BF16),
            pltpu.VMEM((R, 3, cap, emb), BF16),
            pltpu.VMEM((R, 3, cap, emb), BF16),
            sems((2,)),
            sems((R,)), sems((R,)), sems((R,)), sems((R,)), sems((R,)), sems((R,)),
            sems((G,)), sems((G,)), sems((G,)), sems((G,)),
        ],
        compiler_params=pltpu.CompilerParams(
            collective_id=0, has_side_effects=True, vmem_limit_bytes=60 * 1024 * 1024
        ),
        name="embed_step",
    )(idx, tables, w_first, b_first.reshape(1, hidden), w_out.reshape(1, hidden))
    return table_grad, losses.reshape(share)


def solution(mesh):
    placed = (
        P("rows", "grp", None),
        P("rows", "grp", None),
        P("grp", "rows", None),
        P("grp", None),
        P(),
        P(),
        P("rows"),
    )
    return jax.shard_map(
        body,
        mesh=mesh,
        in_specs=placed,
        out_specs=(P("grp", "rows", None), P(("rows", "grp"))),
        check_vma=False,
    )
```

```python
import functools

import jax
import jax.numpy as jnp
from jax import lax
from jax.experimental import pallas as pl
from jax.experimental.pallas import tpu as pltpu
from jax.sharding import PartitionSpec as P

BF16 = jnp.bfloat16
F32 = jnp.float32


def iota(shape, dim):
    return lax.broadcasted_iota(jnp.int32, shape, dim)


def ones_where(mask):
    return jnp.where(mask, 1.0, 0.0).astype(BF16)


def join_bands(bands, starts, width, total):
    cuts = sorted({0, total, *starts, *(min(s + width, total) for s in starts)})
    pieces = []
    for lo, hi in zip(cuts[:-1], cuts[1:]):
        piece = None
        for band, s in zip(bands, starts):
            if s <= lo and hi <= s + width:
                part = band[lo - s : hi - s]
                piece = part if piece is None else piece + part
        pieces.append(piece)
    return jnp.concatenate(pieces, axis=0).astype(BF16)


def mm(a, b):
    return jnp.dot(a, b, preferred_element_type=F32)


def kernel(
    R, G, cap, fgrp, starts, width,
    own_ref, off_ref, lab_ref, tab_hbm, w_hbm, b_ref, wo_ref,
    tg_ref, loss_ref,
    idx_ref, tab, tb, w, col, of, ranked_bf, req_send, req_recv, fet_send, rows, looked,
    p_ref, pt_ref, st_ref, part_f32, part_send, swap_recv, pair_send, pair_recv, gp, rg, g_send, g_recv,
    local_sem, ss0, rs0, ss1, rs1, ss2, rs2, ssp, rsp, ssg, rsg,
):
    me = lax.axis_index("rows")
    mg = lax.axis_index("grp")
    n_rows = tab.shape[1]
    emb = tab.shape[2]
    nl = idx_ref.shape[1]
    per = nl // 3
    bdev = per // fgrp
    share = bdev // G
    r8 = R * 8
    slots = R * width

    total = fet_send.shape[1]
    joined = functools.partial(join_bands, starts=starts, width=width, total=total)
    barrier = pltpu.get_barrier_semaphore()

    def up(k):
        return lax.rem(me + k, R)

    def down(k):
        return lax.rem(me - k + R, R)

    def gup(k):
        return lax.rem(mg + k, G)

    @pl.loop(1, R)
    def _(k):
        pl.semaphore_signal(barrier, inc=1, device_id={"rows": up(k)})

    @pl.loop(1, G)
    def _(k):
        pl.semaphore_signal(barrier, inc=1, device_id={"grp": gup(k)})

    tab_copy = pltpu.make_async_copy(tab_hbm, tab, local_sem.at[0])
    w_copy = pltpu.make_async_copy(w_hbm, w, local_sem.at[1])
    tab_copy.start()
    w_copy.start()

    idx_ref[...] = jnp.zeros_like(idx_ref)
    idx_ref[2:3, 0:bdev] = lab_ref[...]
    for t in range(3):
        for f in range(fgrp):
            lanes = pl.ds(t * per + f * bdev, bdev)
            owner = own_ref[f, t : t + 1, :]
            idx_ref[0:1, lanes] = owner * 8 + t
            idx_ref[1:2, lanes] = off_ref[f, t : t + 1, :]
            idx_ref[3:4, lanes] = owner * width + (t * (cap // 3) - starts[t])
    for j in range(nl // 128):
        col[pl.ds(j * 128, 128), :] = idx_ref[:, pl.ds(j * 128, 128)].T
    for t in range(3):
        at = pl.ds(t * per, per)
        of[at, :] = ones_where(iota((per, n_rows), 1) == col[at, 1:2])
    owner_hot = ones_where(iota((r8, nl), 0) == idx_ref[0:1, :])
    present = mm(owner_hot, of[...]) > 0.5
    before = ones_where(iota((n_rows, n_rows), 0) < iota((n_rows, n_rows), 1))
    ranked = jnp.where(present, mm(ones_where(present), before), -1.0)
    ranked_bf[...] = ranked.astype(BF16)
    req_send[...] = ranked.reshape(R, 8, n_rows)

    pl.semaphore_wait(barrier, R - 1 + G - 1)

    def req_copy(k):
        return pltpu.make_async_remote_copy(
            req_send.at[up(k)], req_recv.at[me], ss0.at[k], rs0.at[k],
            device_id={"rows": up(k)}, device_id_type=pl.DeviceIdType.MESH,
        )

    @pl.loop(1, R)
    def _(k):
        req_copy(k).start()

    tab_copy.wait()
    tb[...] = tab[...].astype(BF16)
    req_recv[me] = req_send[me]

    for t in range(3):
        at = pl.ds(t * per, per)
        own_hot = ones_where(iota((per, r8), 1) == col[at, 0:1])
        picked = mm(own_hot, ranked_bf[...]) * of[at, :].astype(F32)
        slot = jnp.sum(picked, axis=1, keepdims=True) + col[at, 3:4].astype(F32)
        looked[t] = jnp.broadcast_to(slot, (per, emb))

    def fetch(src):
        rank = req_recv[src]
        bands = []
        for t in range(3):
            shift = t * (cap // 3) - starts[t]
            line = (iota((width, n_rows), 0) - shift).astype(F32)
            line = jnp.where(line < 0.0, -2.0, line)
            bands.append(mm(ones_where(line == rank[t : t + 1, :]), tb[t]))
        fet_send[src] = joined(bands)

    def row_copy(k):
        return pltpu.make_async_remote_copy(
            fet_send.at[down(k)], rows.at[me], ss1.at[k], rs1.at[k],
            device_id={"rows": down(k)}, device_id_type=pl.DeviceIdType.MESH,
        )

    @pl.loop(1, R)
    def _(k):
        req_copy(k).wait_recv()
        fetch(down(k))
        row_copy(k).start()

    fetch(me)
    rows[me] = fet_send[me]

    lane_slot = iota((per, slots), 1).astype(F32)
    for t in range(3):
        slot = looked[t]
        p_ref[t] = ones_where(lane_slot == slot[:, 0:1])
        slot_row = slot.T[0:1, :]
        pt_ref[t] = ones_where(iota((slots, per), 0).astype(F32) == slot_row)
    req_cols = req_recv[...].reshape(r8, n_rows).T.astype(BF16)
    row_i = iota((r8, slots), 0)
    col_j = iota((r8, slots), 1)
    first = (row_i >> 3) * width
    slot_in = iota((n_rows, slots), 1) & (width - 1)
    for t in range(3):
        spread = ones_where(((row_i & 7) == t) & (col_j >= first) & (col_j < first + width))
        line = (slot_in - (t * (cap // 3) - starts[t])).astype(F32)
        line = jnp.where(line < 0.0, -2.0, line)
        st_ref[t] = ones_where(mm(req_cols, spread) == line)

    @pl.loop(1, R)
    def _(k):
        row_copy(k).wait_recv()

    for t in range(3):
        looked[t] = mm(p_ref[t], rows[:, starts[t] : starts[t] + width].reshape(slots, emb))
    embedded = (looked[0] * looked[1] + looked[2]).astype(BF16)
    features = jnp.concatenate(
        [embedded[f * bdev : (f + 1) * bdev] for f in range(fgrp)], axis=1
    )
    w_copy.wait()
    partial = mm(features, w[...])
    hidden = partial.shape[1]
    half = G // 2
    side = lax.rem(mg, 2)
    partner = mg + 1 - 2 * side
    mine = lax.div(mg, 2)
    for g in range(G):
        block = partial[g * share : (g + 1) * share]
        part_f32[g % 2, g // 2] = block
        part_send[g % 2, g // 2] = block.astype(BF16)
    swap = pltpu.make_async_remote_copy(
        part_send.at[1 - side], swap_recv, ssp.at[0], rsp.at[0],
        device_id={"grp": partner}, device_id_type=pl.DeviceIdType.MESH,
    )
    swap.start()

    def part_copy(k):
        peer = lax.rem(mg + 2 * k, G)
        return pltpu.make_async_remote_copy(
            pair_send, pair_recv.at[k], ssp.at[k], rsp.at[k],
            device_id={"grp": peer}, device_id_type=pl.DeviceIdType.MESH,
        )

    swap.wait_recv()
    pair = part_f32[side] + swap_recv[...].astype(F32)
    pair_send[...] = pair.astype(BF16)
    for k in range(1, half):
        part_copy(k).start()
    pair = pair + b_ref[...]
    for k in range(1, half):
        part_copy(k).wait_recv()
        pair = pair + pair_recv[k].astype(F32)
    pre = pair.reshape(half * share, hidden)
    sig = jax.nn.sigmoid(pre)
    w_out = wo_ref[...]
    logits = jnp.sum(pre * sig * w_out, axis=1, keepdims=True)
    targets = jnp.concatenate(
        [
            col[pl.ds(pl.multiple_of((2 * j + side) * share, share), share), 2:3]
            for j in range(half)
        ],
        axis=0,
    ).astype(F32)
    grad_logit = jax.nn.sigmoid(logits) - targets
    grad_half = (grad_logit * w_out * (sig * (1.0 + pre * (1.0 - sig)))).astype(BF16)
    gp[side] = grad_half.reshape(half, share, hidden)
    gp_copy = pltpu.make_async_remote_copy(
        gp.at[side], gp.at[side], ssg.at[0], rsg.at[0],
        device_id={"grp": partner}, device_id_type=pl.DeviceIdType.MESH,
    )
    gp_copy.start()
    losses = (
        jnp.maximum(logits, 0.0) + jnp.log1p(jnp.exp(-jnp.abs(logits))) - targets * logits
    )
    diag = iota((half * share, share), 0) - mine * share == iota((half * share, share), 1)
    loss_ref[...] = jnp.sum(jnp.where(diag, losses, 0.0), axis=0, keepdims=True)
    gp_copy.wait_recv()
    grad_pre = jnp.concatenate([gp[g % 2, g // 2] for g in range(G)], axis=0)

    grad_emb = lax.dot_general(
        grad_pre, w[...], (((1,), (1,)), ((), ())),
        preferred_element_type=F32,
    )
    grad_rows = jnp.concatenate(
        [grad_emb[:, f * emb : (f + 1) * emb] for f in range(fgrp)], axis=0
    )
    rg[0] = (grad_rows * looked[1]).astype(BF16)
    rg[1] = (grad_rows * looked[0]).astype(BF16)
    rg[2] = grad_rows.astype(BF16)

    def collect(dst):
        at = pl.ds(pl.multiple_of(dst * width, width), width)
        g_send[dst] = joined([mm(pt_ref[t, at, :], rg[t]) for t in range(3)])

    def grad_copy(k):
        return pltpu.make_async_remote_copy(
            g_send.at[up(k)], g_recv.at[me], ss2.at[k], rs2.at[k],
            device_id={"rows": up(k)}, device_id_type=pl.DeviceIdType.MESH,
        )

    @pl.loop(1, R)
    def _(k):
        collect(up(k))
        grad_copy(k).start()

    collect(me)
    g_recv[me] = g_send[me]

    @pl.loop(1, R)
    def _(k):
        req_copy(k).wait_send()
        row_copy(k).wait_send()

    swap.wait_send()
    gp_copy.wait_send()
    for k in range(1, half):
        part_copy(k).wait_send()

    @pl.loop(1, R)
    def _(k):
        grad_copy(k).wait_recv()

    for t in range(3):
        tg_ref[t] = mm(st_ref[t], g_recv[:, starts[t] : starts[t] + width].reshape(slots, emb))

    @pl.loop(1, R)
    def _(k):
        grad_copy(k).wait_send()


def body(owner, offset, tables, w_first, b_first, w_out, labels):
    R, G = lax.axis_size("rows"), lax.axis_size("grp")
    bdev, fgrp = owner.shape[0], owner.shape[1]
    n_rows, emb = tables.shape[1], tables.shape[2]
    hidden = w_first.shape[1]
    per = bdev * fgrp
    nl = 3 * per
    hot_count = 8 * (per * 7 // (16 * R)) + 8
    uniq = hot_count // 3
    cap = 3 * uniq
    total = -(-cap // 16) * 16
    starts = [t * uniq // 16 * 16 for t in range(3)]
    width = 16
    while any(s + width < (t + 1) * uniq for t, s in enumerate(starts)):
        width *= 2
    total = max(total, max(starts) + width)
    share = bdev // G
    half = G // 2
    slots = R * width

    owner_rows = owner.transpose(1, 2, 0)
    offset_rows = offset.transpose(1, 2, 0)
    vmem = pl.BlockSpec(memory_space=pltpu.VMEM)
    hbm = pl.BlockSpec(memory_space=pl.ANY)
    sems = pltpu.SemaphoreType.DMA
    table_grad, losses = pl.pallas_call(
        functools.partial(kernel, R, G, cap, fgrp, starts, width),
        out_shape=(
            jax.ShapeDtypeStruct((3, n_rows, emb), F32),
            jax.ShapeDtypeStruct((1, share), F32),
        ),
        in_specs=[vmem, vmem, vmem, hbm, hbm, vmem, vmem],
        out_specs=(vmem, vmem),
        scratch_shapes=[
            pltpu.VMEM((8, nl), jnp.int32),
            pltpu.VMEM((3, n_rows, emb), F32),
            pltpu.VMEM((3, n_rows, emb), BF16),
            pltpu.VMEM(w_first.shape, BF16),
            pltpu.VMEM((nl, 8), jnp.int32),
            pltpu.VMEM((nl, n_rows), BF16),
            pltpu.VMEM((R * 8, n_rows), BF16),
            pltpu.VMEM((R, 8, n_rows), F32),
            pltpu.VMEM((R, 8, n_rows), F32),
            pltpu.VMEM((R, total, emb), BF16),
            pltpu.VMEM((R, total, emb), BF16),
            pltpu.VMEM((3, per, emb), F32),
            pltpu.VMEM((3, per, slots), BF16),
            pltpu.VMEM((3, slots, per), BF16),
            pltpu.VMEM((3, n_rows, slots), BF16),
            pltpu.VMEM((2, half, share, hidden), F32),
            pltpu.VMEM((2, half, share, hidden), BF16),
            pltpu.VMEM((half, share, hidden), BF16),
            pltpu.VMEM((half, share, hidden), BF16),
            pltpu.VMEM((half, half, share, hidden), BF16),
            pltpu.VMEM((2, half, share, hidden), BF16),
            pltpu.VMEM((3, per, emb), BF16),
            pltpu.VMEM((R, total, emb), BF16),
            pltpu.VMEM((R, total, emb), BF16),
            sems((2,)),
            sems((R,)), sems((R,)), sems((R,)), sems((R,)), sems((R,)), sems((R,)),
            sems((G,)), sems((G,)), sems((G,)), sems((G,)),
        ],
        compiler_params=pltpu.CompilerParams(
            collective_id=0, has_side_effects=True, vmem_limit_bytes=60 * 1024 * 1024
        ),
        name="embed_step",
    )(owner_rows, offset_rows, labels.reshape(1, bdev), tables, w_first, b_first.reshape(1, hidden), w_out.reshape(1, hidden))
    return table_grad, losses.reshape(share)


def solution(mesh):
    placed = (
        P("rows", "grp", None),
        P("rows", "grp", None),
        P("grp", "rows", None),
        P("grp", None),
        P(),
        P(),
        P("rows"),
    )
    return jax.shard_map(
        body,
        mesh=mesh,
        in_specs=placed,
        out_specs=(P("grp", "rows", None), P(("rows", "grp"))),
        check_vma=False,
    )
```
